768 devices in a mesh: dp: 96 (over y_lo, z, x), seq: 8 (over y_hi, core).
Axes of the slice: x: 4, y: 8 (y_hi: 4, y_lo: 2; y = y_hi * 2 + y_lo), z: 12, core: 2. Of those that a mesh axis runs over, the one named last changes fastest.
Arguments:
- queries: bfloat16 [98304, 2048], P(('dp', 'seq')), may hold values from -6 to 6
- keys: bfloat16 [98304, 2048], P(('dp', 'seq')), may hold values from -6 to 6
- values: bfloat16 [98304, 2048], P(('dp', 'seq')), may hold values from -6 to 6
- q_gain: float32 [2048], replicated, may hold values from 0.25 to 1.75
- k_gain: float32 [2048], replicated, may hold values from 0.25 to 1.75
- out_grad: bfloat16 [98304, 2048], P(('dp', 'seq')), may hold values from -16 to 16
- segments: int32 [96, 1024], P('dp'), may hold values from 0 to 3, never falling along the last dimension, each value on 1 to 512 neighbouring positions
- visible: int32 [96, 1024], P('dp'), may hold values 0 or 1
Outputs:
- attn_out: bfloat16 [98304, 2048], P(('dp', 'seq'))
- query_grad: bfloat16 [98304, 2048], P(('dp', 'seq'))
- key_grad: bfloat16 [98304, 2048], P(('dp', 'seq'))
- value_grad: bfloat16 [98304, 2048], P(('dp', 'seq'))
- q_gain_grad: float32 [2048], replicated
- k_gain_grad: float32 [2048], replicated
The draws below stay inside these ranges and needn't reach their ends.
Inputs may be any that keep to these rules, and one draw needn't show every extreme that they name: `segments`: along each packed sequence the clip numbers never fall; each of the 4 clips holds 1 to 512 slots.
All inputs are finite; a program needn't handle non-finite values. No bound on the sum of `visible` on one device may be relied on, other than what follows from the above.
Results may differ from the reference program's by a relative error of at most 0.012.
The reference program's roundings to bfloat16 on the way (of `prob_half` and `score_grad`) count: a program that leaves them out, or rounds other values in their place, can miss the bound.
Values may be sent and summed in bfloat16 or wider, within the bound.
A program may use at most 64 MiB of HBM per device.

```python
import math
import jax
import jax.numpy as jnp
import numpy as np
from jax import lax

HEADS = 16
D_HEAD = 128
CLIPS = 4
WIDTH = 2048
SEQ_LEN = 1024
TOKENS = 98304
N_DP = 96


def draw_queries(key, part):
    drawn = jax.random.normal(jax.random.fold_in(key, 11), (TOKENS, HEADS * D_HEAD), jnp.float32)
    return jnp.clip(drawn, -6.0, 6.0).astype(jnp.bfloat16)


def draw_keys(key, part):
    drawn = jax.random.normal(jax.random.fold_in(key, 23), (TOKENS, HEADS * D_HEAD), jnp.float32)
    return jnp.clip(drawn, -6.0, 6.0).astype(jnp.bfloat16)


def place_ends(values, stream_key, least, top_value):
    longest = values.shape.index(max(values.shape))
    spots = []
    for shift in (0, 1):
        where = [jax.random.randint(jax.random.fold_in(stream_key, axis), (), 0, length) for axis, length in enumerate(values.shape)]
        where[longest] = (where[longest] + shift) % values.shape[longest]
        spots.append(tuple(where))
    return values.at[spots[0]].set(least).at[spots[1]].set(top_value)


def block_scale(own_key, extent, split, smallest, largest):
    level, own = 1.0, jax.random.fold_in(own_key, 6)
    for axis_at, parts in split:
        steps = jnp.exp(jax.random.uniform(jax.random.fold_in(own, axis_at), (parts,), jnp.float32, smallest / len(split), largest / len(split)))
        level = level * jnp.repeat(steps, extent[axis_at] // parts).reshape([-1 if axis == axis_at else 1 for axis in range(len(extent))])
    return level


def profile(amount, total, most, skew):
    loads = [(1 << 20) // math.isqrt(grade ** skew) + 1 for grade in range(2, amount + 1)]
    spare, holding = total - most - (amount - 1), [1] * (amount - 1)
    while spare > 0:
        movable = [i for i in range(amount - 1) if holding[i] < most]
        mass, left = sum([loads[i] for i in movable]), spare
        for i in movable:
            addition = min(most - holding[i], max(1, left * loads[i] // mass), spare)
            holding[i] = holding[i] + addition
            spare = spare - addition
    return np.array([most] + holding)


def uneven(own_key, count, total, most, slope):
    if count == 2:
        one = jax.random.randint(own_key, (), max(1, total - most), min(most, total - 1) + 1)
        return jnp.stack([one, total - one])
    lengths = jnp.asarray(profile(count, total, most, slope), jnp.int32)
    pairs = (count - 1) // 2
    source_of, receiver = lengths[1:1 + 2 * pairs:2], lengths[2:2 + 2 * pairs:2]
    room = jnp.minimum(source_of - 1, most - receiver)
    shifted = jax.random.randint(jax.random.fold_in(own_key, 1), (pairs,), 0, 1 << 20) % (room + 1)
    lengths = lengths.at[1:1 + 2 * pairs:2].set(source_of - shifted).at[2:2 + 2 * pairs:2].set(receiver + shifted)
    return lengths[jax.random.permutation(jax.random.fold_in(own_key, 2), count)]


def normal_values(key, extent, scale, reach, pieces=(), kind=jnp.bfloat16):
    loudness = block_scale(key, extent, pieces, -0.22, 0.18) if pieces else 1.0
    values = jax.random.normal(key, extent, jnp.float32) * scale * loudness
    return jnp.minimum(jnp.maximum(values, -reach), reach).astype(kind)


def setup_inputs(seed: int = 0) -> dict:
    splits = jax.random.split(jax.random.key(seed), 9)
    queries = draw_queries(jax.random.fold_in(splits[8], 71), 0)
    keys = draw_keys(jax.random.fold_in(splits[8], 71), 0)
    values = normal_values(splits[2], (TOKENS, WIDTH), 1.0, 6.0, ((0, 768),))
    q_gain = jnp.clip(1.0 + 0.15 * jax.random.normal(splits[3], (WIDTH,), jnp.float32), 0.25, 1.75)
    k_gain = jnp.clip(1.0 + 0.15 * jax.random.normal(splits[4], (WIDTH,), jnp.float32), 0.25, 1.75)
    out_grad = normal_values(splits[5], (TOKENS, WIDTH), 4.0, 16.0, ((0, 768),))
    segments = jax.vmap(lambda own: jnp.searchsorted(jnp.cumsum(uneven(own, CLIPS, SEQ_LEN, SEQ_LEN // 2, 2)), jnp.arange(SEQ_LEN), side="right"))(jax.random.split(splits[6], N_DP)).reshape((N_DP, SEQ_LEN)).astype(jnp.int32)
    visible = place_ends((jax.random.randint(splits[7], (N_DP, SEQ_LEN), 0, 5) < 4).astype(jnp.int32), jax.random.fold_in(splits[7], 1), 0, 1)
    return dict(queries=queries, keys=keys, values=values, q_gain=q_gain, k_gain=k_gain, out_grad=out_grad, segments=segments, visible=visible)


epsilon = 1e-06

def normalize(raw_rows, gain_vec):
    raw_f32 = raw_rows.astype(jnp.float32)
    inv_rms = lax.rsqrt(lax.optimization_barrier(jnp.mean(raw_f32 * raw_f32, axis=-1, keepdims=True)) + epsilon)
    return ((raw_f32 * inv_rms * gain_vec).astype(jnp.bfloat16), inv_rms)

def norm_back(raw_rows, inv_rms, gain_vec, grad_norm):
    raw_f32 = raw_rows.astype(jnp.float32)
    grad_f32 = grad_norm.astype(jnp.float32)
    scaled_grad = gain_vec * grad_f32
    mean_term = lax.optimization_barrier(jnp.mean(scaled_grad * raw_f32, axis=-1, keepdims=True))
    grad_raw = inv_rms * scaled_grad - raw_f32 * inv_rms ** 3 * mean_term
    return (grad_raw.astype(jnp.bfloat16), lax.optimization_barrier(jnp.sum(grad_f32 * raw_f32 * inv_rms, axis=0)))

def attend(items):
    q_norm, k_norm, val_rows, grad_rows, seg_row, vis_row = items
    seq_rows = q_norm.shape[0]
    score_scale = D_HEAD ** (-0.5)
    q_three = q_norm.reshape(seq_rows, HEADS, D_HEAD).astype(jnp.float32)
    k_three = k_norm.reshape(seq_rows, HEADS, D_HEAD).astype(jnp.float32)
    v_three = val_rows.reshape(seq_rows, HEADS, D_HEAD).astype(jnp.float32)
    grad_three = grad_rows.reshape(seq_rows, HEADS, D_HEAD).astype(jnp.float32)
    positions = jnp.arange(seq_rows, dtype=jnp.int32)
    allowed = (seg_row[:, None] == seg_row[None, :]) & ((vis_row[None, :] == 1) | (positions[:, None] == positions[None, :]))
    scores = jnp.einsum('shd,thd->hst', q_three, k_three) * score_scale
    scores = jnp.where(allowed[None], scores, -1e+30)
    row_max = lax.optimization_barrier(jnp.max(scores, axis=-1, keepdims=True))
    weights = jnp.exp(scores - row_max)
    attn_prob = weights / lax.optimization_barrier(jnp.sum(weights, axis=-1, keepdims=True))
    prob_half = lax.optimization_barrier(attn_prob.astype(jnp.bfloat16)).astype(jnp.float32)
    attn_out = jnp.einsum('hst,thd->shd', prob_half, v_three).reshape(seq_rows, WIDTH).astype(jnp.bfloat16)
    dprob = jnp.einsum('shd,thd->hst', grad_three, v_three)
    val_grad = jnp.einsum('hst,shd->thd', prob_half, grad_three).reshape(seq_rows, WIDTH).astype(jnp.bfloat16)
    row_dot = lax.optimization_barrier(jnp.sum(attn_prob * dprob, axis=-1, keepdims=True))
    score_grad = attn_prob * (dprob - row_dot) * score_scale
    score_grad = lax.optimization_barrier(score_grad.astype(jnp.bfloat16)).astype(jnp.float32)
    q_grad = jnp.einsum('hst,thd->shd', score_grad, k_three).reshape(seq_rows, WIDTH).astype(jnp.bfloat16)
    k_grad = jnp.einsum('hst,shd->thd', score_grad, q_three).reshape(seq_rows, WIDTH).astype(jnp.bfloat16)
    return (attn_out, q_grad, k_grad, val_grad)

def reference(queries, keys, values, q_gain, k_gain, out_grad, segments, visible):
    q_norm, q_inv = normalize(queries, q_gain)
    k_norm, k_inv = normalize(keys, k_gain)

    def packed(array):
        return array.reshape(N_DP, SEQ_LEN, WIDTH)
    results = lax.map(attend, (packed(q_norm), packed(k_norm), packed(values), packed(out_grad), segments, visible))
    attn_out, q_grad, k_grad, val_grad = [packed_out.reshape(TOKENS, WIDTH) for packed_out in results]
    query_grad, q_gain_grad = norm_back(queries, q_inv, q_gain, q_grad)
    key_grad, k_gain_grad = norm_back(keys, k_inv, k_gain, k_grad)
    return (attn_out, query_grad, key_grad, val_grad, q_gain_grad, k_gain_grad)
```

```python
import functools

import jax
import jax.numpy as jnp
from jax import lax
from jax.experimental import pallas as pl
from jax.experimental.pallas import tpu as pltpu
from jax.sharding import Mesh
from jax.sharding import PartitionSpec as P

D_HEAD = 128
DP_SEQ = ("dp_0", "dp_1", "dp_2", "seq_0", "seq_1")
DP = ("dp_0", "dp_1", "dp_2")
MESH = pl.DeviceIdType.MESH

epsilon = 1e-06
N_SEQ = 8
ROWS = 128
LEN = 1024
WIDTH = 2048
BLOCK = 256
SCALE = D_HEAD ** (-0.5)
LOG2E = 1.4426950408889634
SLOTS = 16


def nt(a, b):
    return lax.dot_general(a, b, (((1,), (1,)), ((), ())), preferred_element_type=jnp.float32)


def tn(a, b):
    return lax.dot_general(a, b, (((0,), (0,)), ((), ())), preferred_element_type=jnp.float32)


def nn(a, b):
    return lax.dot_general(a, b, (((1,), (0,)), ((), ())), preferred_element_type=jnp.float32)


def wide(gain_ref):
    return jnp.concatenate([gain_ref[r : r + 1, :] for r in range(WIDTH // 128)], axis=1)


def kernel(
    q_ref, k_ref, v_ref, g_ref, qg_ref, kg_ref, seg_ref, vis_ref,
    o_ref, dq_ref, dk_ref, dv_ref, gq_ref, gk_ref,
    qn, kn, qi, ki, rx, tx, rdq, rdk, code, acc_k, acc_v, part, gx, gz, gy,
    in_send, in_recv, out_send, out_recv, g_send, g_recv,
):
    ylo, z, x = lax.axis_index("dp_0"), lax.axis_index("dp_1"), lax.axis_index("dp_2")
    chip, core = lax.axis_index("seq_0"), lax.axis_index("seq_1")
    me = chip * 2 + core

    barrier = pltpu.get_barrier_semaphore()

    def greet(device):
        pl.semaphore_signal(barrier, inc=1, device_id=device, device_id_type=MESH)

    def member(step):
        other = lax.rem(me + step, N_SEQ)
        return other, {"seq_0": other // 2, "seq_1": lax.rem(other, 2)}

    def across(step):
        other = lax.rem(ylo * N_SEQ + me + step, SLOTS)
        return {
            "dp_0": other // N_SEQ,
            "seq_0": lax.rem(other, N_SEQ) // 2,
            "seq_1": lax.rem(other, 2),
        }

    x_peers = [{"dp_2": lax.rem(x + d, 4)} for d in range(1, 4)]
    z_peers = [{"dp_1": lax.rem(z + d, 12)} for d in range(1, 12)]
    y_peers = [across(d) for d in range(1, SLOTS)]
    everyone = y_peers + x_peers + z_peers
    for device in everyone:
        greet(device)

    def normalize(raw_ref, gain, out, inv_ref):
        def rows_of(i, _):
            rows = pl.ds(pl.multiple_of(i * 16, 16), 16)
            raw = raw_ref[rows, :].astype(jnp.float32)
            inv = lax.rsqrt(jnp.mean(raw * raw, axis=-1, keepdims=True) + epsilon)
            inv_ref[rows, :] = jnp.broadcast_to(inv, (16, 128))
            out[rows, :] = (raw * inv * gain).astype(jnp.bfloat16)
            return 0

        lax.fori_loop(0, ROWS // 16, rows_of, 0)

    part[...] = jnp.zeros_like(part)
    q_gain, k_gain = wide(qg_ref), wide(kg_ref)
    normalize(q_ref, q_gain, qn, qi)
    normalize(k_ref, k_gain, kn, ki)
    sources = (qn, kn, v_ref, g_ref)
    my_rows = pl.ds(pl.multiple_of(me * ROWS, ROWS), ROWS)

    def columns(device, h):
        return pl.ds(pl.multiple_of(device * 256 + h * 128, 128), 128)

    pl.semaphore_wait(barrier, len(everyone))

    for h in range(2):
        for a in range(4):
            for step in (2, 3, 6, 7, 4, 5, 1):
                other, device = member(step)
                pltpu.make_async_remote_copy(
                    src_ref=sources[a].at[:, columns(other, h)],
                    dst_ref=rx.at[a, h, my_rows],
                    send_sem=in_send.at[a, h],
                    recv_sem=in_recv.at[a, h],
                    device_id=device,
                    device_id_type=MESH,
                ).start()
    for h in range(2):
        for a in range(4):
            rx[a, h, my_rows, :] = sources[a][:, columns(me, h)]

    seg_row = seg_ref[...].astype(jnp.float32)
    key_row = jnp.where(vis_ref[...] == 1, seg_row, -1.0)
    for j in range(LEN // 128):
        piece = jnp.broadcast_to(key_row[:, j * 128 : (j + 1) * 128], (128, 128))
        code[j * 128 : (j + 1) * 128, :] = piece.T

    def of_all(a, h, sends, recvs):
        return pltpu.make_async_remote_copy(
            src_ref=rx.at[a, h, pl.ds(0, 7 * ROWS)],
            dst_ref=rx.at[a, h, pl.ds(0, 7 * ROWS)],
            send_sem=sends.at[a, h],
            recv_sem=recvs.at[a, h],
            device_id=member(1)[1],
            device_id_type=MESH,
        )

    landing = (o_ref, rdq, rdk, dv_ref)

    def send_out(a, h, other):
        pltpu.make_async_remote_copy(
            src_ref=tx.at[a, h, pl.ds(pl.multiple_of(other * ROWS, ROWS), ROWS)],
            dst_ref=landing[a].at[:, columns(me, h)],
            send_sem=out_send.at[a, h],
            recv_sem=out_recv.at[a, h],
            device_id={"seq_0": other // 2, "seq_1": lax.rem(other, 2)},
            device_id_type=MESH,
        ).start()

    def keep_own(a, h):
        landing[a][:, columns(me, h)] = tx[a, h, my_rows, :]

    for h in range(2):
        for a in range(4):
            of_all(a, h, in_send, in_recv).wait_recv()
        acc_k[...] = jnp.zeros_like(acc_k)
        acc_v[...] = jnp.zeros_like(acc_v)

        def block(t, gain_sum):
            at_chip = lax.rem(chip + 1 + t, 4)
            start = pl.multiple_of(at_chip * BLOCK, BLOCK)
            rows = pl.ds(start, BLOCK)
            q_i, g_i = rx[0, h, rows, :], rx[3, h, rows, :]
            keys, vals = rx[1, h], rx[2, h]
            seg_i = seg_ref[:, rows].astype(jnp.float32)
            k_code = code[...]
            k_code = jnp.concatenate([k_code, k_code], axis=1)
            key_at = lax.broadcasted_iota(jnp.int32, (LEN, BLOCK), 0)
            query_at = lax.broadcasted_iota(jnp.int32, (LEN, BLOCK), 1) + start
            allowed = (k_code == seg_i) | (key_at == query_at)
            scores = jnp.where(allowed, nt(keys, q_i), -1e30)
            top = jnp.max(scores, axis=0, keepdims=True)
            weights = jnp.exp2((scores - top) * (SCALE * LOG2E))
            prob = weights * (1.0 / jnp.sum(weights, axis=0, keepdims=True))
            half = prob.astype(jnp.bfloat16)
            tx[0, h, rows, :] = tn(vals, half).T.astype(jnp.bfloat16)
            dprob = nt(vals, g_i)
            dot = jnp.sum(prob * dprob, axis=0, keepdims=True)
            grad = (prob * (dprob - dot) * SCALE).astype(jnp.bfloat16)
            dq_i = tn(keys, grad).T.astype(jnp.bfloat16)
            tx[1, h, rows, :] = dq_i
            acc_v[...] += nn(half, g_i)
            acc_k[...] += nn(grad, q_i)
            for c in range(2):
                other = at_chip * 2 + c

                @pl.when(other != me)
                def _():
                    send_out(0, h, other)
                    send_out(1, h, other)

            return gain_sum + jnp.sum(
                dq_i.astype(jnp.float32) * q_i.astype(jnp.float32), axis=0, keepdims=True
            )

        q_sum = lax.fori_loop(0, LEN // BLOCK, block, jnp.zeros((1, D_HEAD), jnp.float32))
        tx[2, h] = acc_k[...].astype(jnp.bfloat16)
        tx[3, h] = acc_v[...].astype(jnp.bfloat16)
        for a in (2, 3):
            for step in (2, 3, 6, 7, 4, 5, 1):
                send_out(a, h, member(step)[0])
        for a in range(4):
            keep_own(a, h)
        k_sum = jnp.sum(
            tx[2, h].astype(jnp.float32) * rx[1, h].astype(jnp.float32), axis=0, keepdims=True
        )
        part[h : h + 1, :] = q_sum / qg_ref[pl.ds(me * 2 + h, 1), :]
        part[2 + h : 3 + h, :] = k_sum / kg_ref[pl.ds(me * 2 + h, 1), :]

    def spread(slot, peers, sem):
        copies = []
        for device in peers:
            pltpu.make_async_remote_copy(
                src_ref=slot, dst_ref=slot, send_sem=g_send.at[sem], recv_sem=g_recv.at[sem],
                device_id=device, device_id_type=MESH,
            ).start()

    def settle(slots, peers, sem):
        copy = pltpu.make_async_remote_copy(
            src_ref=slots.at[pl.ds(0, len(peers))], dst_ref=slots.at[pl.ds(0, len(peers))],
            send_sem=g_send.at[sem], recv_sem=g_recv.at[sem],
            device_id=peers[0], device_id_type=MESH,
        )
        copy.wait_recv()
        copy.wait_send()

    gx[x] = part[...]
    spread(gx.at[x], x_peers, 0)
    settle(gx, x_peers, 0)
    gz[z] = (gx[0] + gx[1]) + (gx[2] + gx[3])
    spread(gz.at[z], z_peers, 1)
    settle(gz, z_peers, 1)
    total = gz[0]
    for i in range(1, 12):
        total = total + gz[i]
    slot = ylo * N_SEQ + me
    gy[slot] = total
    spread(gy.at[slot], y_peers, 2)

    def norm_back(raw_ref, inv_ref, gain, grads, out):
        def rows_of(i, _):
            rows = pl.ds(pl.multiple_of(i * 16, 16), 16)
            raw = raw_ref[rows, :].astype(jnp.float32)
            inv = inv_ref[rows, :][:, 0:1]
            scaled = gain * grads[rows, :].astype(jnp.float32)
            mean_term = jnp.mean(scaled * raw, axis=-1, keepdims=True)
            out[rows, :] = (inv * scaled - raw * (inv * inv * inv * mean_term)).astype(jnp.bfloat16)
            return 0

        lax.fori_loop(0, ROWS // 16, rows_of, 0)

    for h in range(2):
        of_all(1, h, out_send, out_recv).wait_recv()
    norm_back(q_ref, qi, q_gain, rdq, dq_ref)
    for h in range(2):
        of_all(2, h, out_send, out_recv).wait_recv()
    norm_back(k_ref, ki, k_gain, rdk, dk_ref)
    for a in (0, 3):
        for h in range(2):
            of_all(a, h, out_send, out_recv).wait_recv()
    settle(gy, y_peers, 2)
    for s in range(N_SEQ):
        both = gy[s] + gy[N_SEQ + s]
        gq_ref[2 * s : 2 * s + 2, :] = both[0:2, :]
        gk_ref[2 * s : 2 * s + 2, :] = both[2:4, :]
    for h in range(2):
        for a in range(4):
            of_all(a, h, in_send, in_recv).wait_send()
            of_all(a, h, out_send, out_recv).wait_send()


def per_device(queries, keys, values, q_gain, k_gain, out_grad, segments, visible):
    vmem = pl.BlockSpec(memory_space=pltpu.VMEM)
    rows = jax.ShapeDtypeStruct((ROWS, WIDTH), jnp.bfloat16)
    gains = jax.ShapeDtypeStruct((WIDTH // 128, 128), jnp.float32)
    dma = pltpu.SemaphoreType.DMA
    bf16, f32 = jnp.bfloat16, jnp.float32
    attn_out, query_grad, key_grad, value_grad, gq, gk = pl.pallas_call(
        kernel,
        out_shape=(rows, rows, rows, rows, gains, gains),
        in_specs=[vmem] * 8,
        out_specs=[vmem] * 6,
        scratch_shapes=[
            pltpu.VMEM((ROWS, WIDTH), bf16),
            pltpu.VMEM((ROWS, WIDTH), bf16),
            pltpu.VMEM((ROWS, 128), f32),
            pltpu.VMEM((ROWS, 128), f32),
            pltpu.VMEM((4, 2, LEN, D_HEAD), bf16),
            pltpu.VMEM((4, 2, LEN, D_HEAD), bf16),
            pltpu.VMEM((ROWS, WIDTH), bf16),
            pltpu.VMEM((ROWS, WIDTH), bf16),
            pltpu.VMEM((LEN, 128), f32),
            pltpu.VMEM((LEN, D_HEAD), f32),
            pltpu.VMEM((LEN, D_HEAD), f32),
            pltpu.VMEM((8, 128), f32),
            pltpu.VMEM((4, 8, 128), f32),
            pltpu.VMEM((12, 8, 128), f32),
            pltpu.VMEM((SLOTS, 8, 128), f32),
            dma((4, 2)), dma((4, 2)), dma((4, 2)), dma((4, 2)), dma((3,)), dma((3,)),
        ],
        compiler_params=pltpu.CompilerParams(
            collective_id=0, has_side_effects=True, vmem_limit_bytes=48 * 2**20
        ),
        name="packed_attention",
    )(
        queries, keys, values, out_grad,
        q_gain.reshape(WIDTH // 128, 128), k_gain.reshape(WIDTH // 128, 128),
        segments, visible,
    )
    return (attn_out, query_grad, key_grad, value_grad, gq.reshape(WIDTH), gk.reshape(WIDTH))


def solution(mesh):
    finer = Mesh(mesh.devices.reshape(2, 12, 4, 4, 2), ("dp_0", "dp_1", "dp_2", "seq_0", "seq_1"))
    placed = (
        P(DP_SEQ, None),
        P(DP_SEQ, None),
        P(DP_SEQ, None),
        P(),
        P(),
        P(DP_SEQ, None),
        P(DP, None),
        P(DP, None),
    )
    return jax.shard_map(
        per_device,
        mesh=finer,
        in_specs=placed,
        out_specs=(P(DP_SEQ, None), P(DP_SEQ, None), P(DP_SEQ, None), P(DP_SEQ, None), P(), P()),
        check_vma=False,
    )
```

```python
import functools

import jax
import jax.numpy as jnp
from jax import lax
from jax.experimental import pallas as pl
from jax.experimental.pallas import tpu as pltpu
from jax.sharding import Mesh
from jax.sharding import PartitionSpec as P

D_HEAD = 128
DP_SEQ = ("dp_0", "dp_1", "dp_2", "seq_0", "seq_1")
DP = ("dp_0", "dp_1", "dp_2")
MESH = pl.DeviceIdType.MESH

epsilon = 1e-06
N_SEQ = 8
ROWS = 128
LEN = 1024
WIDTH = 2048
BLOCK = 256
SCALE = D_HEAD ** (-0.5)
LOG2E = 1.4426950408889634
SLOTS = 16


def nt(a, b):
    return lax.dot_general(a, b, (((1,), (1,)), ((), ())), preferred_element_type=jnp.float32)


def tn(a, b):
    return lax.dot_general(a, b, (((0,), (0,)), ((), ())), preferred_element_type=jnp.float32)


def nn(a, b):
    return lax.dot_general(a, b, (((1,), (0,)), ((), ())), preferred_element_type=jnp.float32)


def wide(gain_ref):
    return jnp.concatenate([gain_ref[r : r + 1, :] for r in range(WIDTH // 128)], axis=1)


def kernel(
    q_hbm, k_hbm, v_hbm, g_hbm, qg_hbm, kg_hbm, seg_hbm, vis_hbm,
    o_ref, dq_ref, dk_ref, dv_ref, gq_ref, gk_ref,
    q_ref, k_ref, v_ref, g_ref, qg_ref, kg_ref, seg_ref, vis_ref,
    qn, kn, qi, ki, rx, tx, rdq, rdk, code, acc_k, acc_v, part, gx, gz, gy,
    in_send, in_recv, out_send, out_recv, g_send, g_recv, load_sem, ready, line, go,
):
    ylo, z, x = lax.axis_index("dp_0"), lax.axis_index("dp_1"), lax.axis_index("dp_2")
    chip, core = lax.axis_index("seq_0"), lax.axis_index("seq_1")
    me = chip * 2 + core

    loads = [
        pltpu.make_async_copy(source, target, load_sem.at[i])
        for i, (source, target) in enumerate(
            (
                (qg_hbm, qg_ref), (q_hbm, q_ref), (kg_hbm, kg_ref), (k_hbm, k_ref),
                (v_hbm, v_ref), (g_hbm, g_ref), (seg_hbm, seg_ref), (vis_hbm, vis_ref),
            )
        )
    ]
    for load in loads:
        load.start()

    barrier = pltpu.get_barrier_semaphore()
    leader = me == 0

    def greet(device):
        pl.semaphore_signal(barrier, inc=1, device_id=device, device_id_type=MESH)

    def member(step):
        other = lax.rem(me + step, N_SEQ)
        return other, {"seq_0": other // 2, "seq_1": lax.rem(other, 2)}

    def across(step):
        other = lax.rem(ylo * N_SEQ + me + step, SLOTS)
        return {
            "dp_0": other // N_SEQ,
            "seq_0": lax.rem(other, N_SEQ) // 2,
            "seq_1": lax.rem(other, 2),
        }

    x_peers = [{"dp_2": lax.rem(x + d, 4)} for d in range(1, 4)]
    z_peers = [{"dp_1": lax.rem(z + d, 12)} for d in range(1, 12)]
    y_peers = [across(d) for d in range(1, SLOTS)]
    leaders = x_peers + z_peers + [{"dp_0": 1 - ylo}]
    for step in range(1, N_SEQ):
        other, device = member(step)

        @pl.when(other != 0)
        def _():
            greet(device)

    @pl.when(leader)
    def _():
        for device in leaders:
            greet(device)

    def normalize(raw_ref, gain, out, inv_ref):
        def rows_of(i, _):
            rows = pl.ds(pl.multiple_of(i * 16, 16), 16)
            raw = raw_ref[rows, :].astype(jnp.float32)
            inv = lax.rsqrt(jnp.mean(raw * raw, axis=-1, keepdims=True) + epsilon)
            inv_ref[rows, :] = jnp.broadcast_to(inv, (16, 128))
            out[rows, :] = (raw * inv * gain).astype(jnp.bfloat16)
            return 0

        lax.fori_loop(0, ROWS // 16, rows_of, 0)

    part[...] = jnp.zeros_like(part)
    loads[0].wait()
    loads[1].wait()
    q_gain = wide(qg_ref)
    normalize(q_ref, q_gain, qn, qi)
    loads[2].wait()
    loads[3].wait()
    k_gain = wide(kg_ref)
    normalize(k_ref, k_gain, kn, ki)
    for load in loads[4:]:
        load.wait()
    sources = (qn, kn, v_ref, g_ref)
    my_rows = pl.ds(pl.multiple_of(me * ROWS, ROWS), ROWS)

    def columns(device, h):
        return pl.ds(pl.multiple_of(device * 256 + h * 128, 128), 128)

    @pl.when(me != 0)
    def _():
        pl.semaphore_wait(barrier, N_SEQ - 1)
        pl.semaphore_signal(
            ready, inc=1, device_id={"seq_0": 0, "seq_1": 0}, device_id_type=MESH
        )

    @pl.when(leader)
    def _():
        pl.semaphore_wait(ready, N_SEQ - 1)

    for h in range(2):
        for a in range(4):
            for step in (2, 3, 6, 7, 4, 5, 1):
                other, device = member(step)
                pltpu.make_async_remote_copy(
                    src_ref=sources[a].at[:, columns(other, h)],
                    dst_ref=rx.at[a, h, my_rows],
                    send_sem=in_send.at[a, h],
                    recv_sem=in_recv.at[a, h],
                    device_id=device,
                    device_id_type=MESH,
                ).start()
    for h in range(2):
        for a in range(4):
            rx[a, h, my_rows, :] = sources[a][:, columns(me, h)]

    seg_row = seg_ref[...].astype(jnp.float32)
    key_row = jnp.where(vis_ref[...] == 1, seg_row, -1.0)
    for j in range(LEN // 128):
        piece = jnp.broadcast_to(key_row[:, j * 128 : (j + 1) * 128], (128, 128))
        code[j * 128 : (j + 1) * 128, :] = piece.T

    def of_all(a, h, sends, recvs):
        return pltpu.make_async_remote_copy(
            src_ref=rx.at[a, h, pl.ds(0, 7 * ROWS)],
            dst_ref=rx.at[a, h, pl.ds(0, 7 * ROWS)],
            send_sem=sends.at[a, h],
            recv_sem=recvs.at[a, h],
            device_id=member(1)[1],
            device_id_type=MESH,
        )

    landing = (o_ref, rdq, rdk, dv_ref)

    def send_out(a, h, other):
        pltpu.make_async_remote_copy(
            src_ref=tx.at[a, h, pl.ds(pl.multiple_of(other * ROWS, ROWS), ROWS)],
            dst_ref=landing[a].at[:, columns(me, h)],
            send_sem=out_send.at[a, h],
            recv_sem=out_recv.at[a, h],
            device_id={"seq_0": other // 2, "seq_1": lax.rem(other, 2)},
            device_id_type=MESH,
        ).start()

    def send_all(a, h):
        for step in (2, 3, 6, 7, 4, 5, 1):
            send_out(a, h, member(step)[0])

    def keep_own(a, h):
        landing[a][:, columns(me, h)] = tx[a, h, my_rows, :]

    for h in range(2):
        for a in range(4):
            of_all(a, h, in_send, in_recv).wait_recv()
        if h == 1:
            for a in range(4):
                send_all(a, 0)
        acc_k[...] = jnp.zeros_like(acc_k)
        acc_v[...] = jnp.zeros_like(acc_v)

        def block(t, gain_sum):
            at_chip = lax.rem(chip + 1 + t, 4)
            start = pl.multiple_of(at_chip * BLOCK, BLOCK)
            rows = pl.ds(start, BLOCK)
            q_i, g_i = rx[0, h, rows, :], rx[3, h, rows, :]
            keys, vals = rx[1, h], rx[2, h]
            seg_i = seg_ref[:, rows].astype(jnp.float32)
            k_code = code[...]
            k_code = jnp.concatenate([k_code, k_code], axis=1)
            key_at = lax.broadcasted_iota(jnp.int32, (LEN, BLOCK), 0)
            query_at = lax.broadcasted_iota(jnp.int32, (LEN, BLOCK), 1) + start
            allowed = (k_code == seg_i) | (key_at == query_at)
            scores = jnp.where(allowed, nt(keys, q_i), -1e30)
            top = jnp.max(scores, axis=0, keepdims=True)
            weights = jnp.exp2((scores - top) * (SCALE * LOG2E))
            prob = weights * (1.0 / jnp.sum(weights, axis=0, keepdims=True))
            half = prob.astype(jnp.bfloat16)
            tx[0, h, rows, :] = tn(vals, half).T.astype(jnp.bfloat16)
            dprob = nt(vals, g_i)
            dot = jnp.sum(prob * dprob, axis=0, keepdims=True)
            grad = (prob * (dprob - dot) * SCALE).astype(jnp.bfloat16)
            dq_i = tn(keys, grad).T.astype(jnp.bfloat16)
            tx[1, h, rows, :] = dq_i
            acc_v[...] += nn(half, g_i)
            acc_k[...] += nn(grad, q_i)
            if h == 1:
                for c in range(2):
                    other = at_chip * 2 + c

                    @pl.when(other != me)
                    def _():
                        send_out(0, h, other)
                        send_out(1, h, other)

            return gain_sum + jnp.sum(
                dq_i.astype(jnp.float32) * q_i.astype(jnp.float32), axis=0, keepdims=True
            )

        q_sum = lax.fori_loop(0, LEN // BLOCK, block, jnp.zeros((1, D_HEAD), jnp.float32))
        tx[2, h] = acc_k[...].astype(jnp.bfloat16)
        tx[3, h] = acc_v[...].astype(jnp.bfloat16)
        if h == 1:
            for a in (2, 3):
                send_all(a, h)
        for a in range(4):
            keep_own(a, h)
        k_sum = jnp.sum(
            tx[2, h].astype(jnp.float32) * rx[1, h].astype(jnp.float32), axis=0, keepdims=True
        )
        if h == 0:

            @pl.when(leader)
            def _():
                pl.semaphore_wait(barrier, len(leaders))
                for device in leaders:
                    pl.semaphore_signal(line, inc=1, device_id=device, device_id_type=MESH)

        part[h : h + 1, :] = q_sum / qg_ref[pl.ds(me * 2 + h, 1), :]
        part[2 + h : 3 + h, :] = k_sum / kg_ref[pl.ds(me * 2 + h, 1), :]

    def spread(slot, peers, sem):
        copies = []
        for device in peers:
            pltpu.make_async_remote_copy(
                src_ref=slot, dst_ref=slot, send_sem=g_send.at[sem], recv_sem=g_recv.at[sem],
                device_id=device, device_id_type=MESH,
            ).start()

    def settle(slots, peers, sem):
        copy = pltpu.make_async_remote_copy(
            src_ref=slots.at[pl.ds(0, len(peers))], dst_ref=slots.at[pl.ds(0, len(peers))],
            send_sem=g_send.at[sem], recv_sem=g_recv.at[sem],
            device_id=peers[0], device_id_type=MESH,
        )
        copy.wait_recv()
        copy.wait_send()

    @pl.when(leader)
    def _():
        pl.semaphore_wait(line, len(leaders))
        for step in range(1, N_SEQ):
            pl.semaphore_signal(go, inc=1, device_id=member(step)[1], device_id_type=MESH)

    @pl.when(me != 0)
    def _():
        pl.semaphore_wait(go, 1)

    gx[x] = part[...]
    spread(gx.at[x], x_peers, 0)
    settle(gx, x_peers, 0)
    gz[z] = (gx[0] + gx[1]) + (gx[2] + gx[3])
    spread(gz.at[z], z_peers, 1)
    settle(gz, z_peers, 1)
    total = gz[0]
    for i in range(1, 12):
        total = total + gz[i]
    slot = ylo * N_SEQ + me
    gy[slot] = total
    spread(gy.at[slot], y_peers, 2)

    def norm_back(raw_ref, inv_ref, gain, grads, out):
        def rows_of(i, _):
            rows = pl.ds(pl.multiple_of(i * 16, 16), 16)
            raw = raw_ref[rows, :].astype(jnp.float32)
            inv = inv_ref[rows, :][:, 0:1]
            scaled = gain * grads[rows, :].astype(jnp.float32)
            mean_term = jnp.mean(scaled * raw, axis=-1, keepdims=True)
            out[rows, :] = (inv * scaled - raw * (inv * inv * inv * mean_term)).astype(jnp.bfloat16)
            return 0

        lax.fori_loop(0, ROWS // 16, rows_of, 0)

    for h in range(2):
        of_all(1, h, out_send, out_recv).wait_recv()
    norm_back(q_ref, qi, q_gain, rdq, dq_ref)
    for h in range(2):
        of_all(2, h, out_send, out_recv).wait_recv()
    norm_back(k_ref, ki, k_gain, rdk, dk_ref)
    for a in (0, 3):
        for h in range(2):
            of_all(a, h, out_send, out_recv).wait_recv()
    settle(gy, y_peers, 2)
    for s in range(N_SEQ):
        both = gy[s] + gy[N_SEQ + s]
        gq_ref[2 * s : 2 * s + 2, :] = both[0:2, :]
        gk_ref[2 * s : 2 * s + 2, :] = both[2:4, :]
    for h in range(2):
        for a in range(4):
            of_all(a, h, in_send, in_recv).wait_send()
            of_all(a, h, out_send, out_recv).wait_send()


def store(*refs):
    n = 6
    sources, targets, sem = refs[:n], refs[n : 2 * n], refs[2 * n]
    copies = [pltpu.make_async_copy(sources[i], targets[i], sem.at[i]) for i in range(n)]
    for copy in copies:
        copy.start()
    for copy in copies:
        copy.wait()


def per_device(queries, keys, values, q_gain, k_gain, out_grad, segments, visible):
    vmem = pl.BlockSpec(memory_space=pltpu.VMEM)
    rows = jax.ShapeDtypeStruct((ROWS, WIDTH), jnp.bfloat16)
    gains = jax.ShapeDtypeStruct((WIDTH // 128, 128), jnp.float32)
    dma = pltpu.SemaphoreType.DMA
    bf16, f32 = jnp.bfloat16, jnp.float32
    hbm = pl.BlockSpec(memory_space=pltpu.HBM)
    outs = (rows, rows, rows, rows, gains, gains)
    made = pl.pallas_call(
        kernel,
        out_shape=outs,
        in_specs=[hbm] * 8,
        out_specs=[vmem] * 6,
        scratch_shapes=[
            pltpu.VMEM((ROWS, WIDTH), bf16),
            pltpu.VMEM((ROWS, WIDTH), bf16),
            pltpu.VMEM((ROWS, WIDTH), bf16),
            pltpu.VMEM((ROWS, WIDTH), bf16),
            pltpu.VMEM((WIDTH // 128, 128), f32),
            pltpu.VMEM((WIDTH // 128, 128), f32),
            pltpu.VMEM((1, LEN), jnp.int32),
            pltpu.VMEM((1, LEN), jnp.int32),
            pltpu.VMEM((ROWS, WIDTH), bf16),
            pltpu.VMEM((ROWS, WIDTH), bf16),
            pltpu.VMEM((ROWS, 128), f32),
            pltpu.VMEM((ROWS, 128), f32),
            pltpu.VMEM((4, 2, LEN, D_HEAD), bf16),
            pltpu.VMEM((4, 2, LEN, D_HEAD), bf16),
            pltpu.VMEM((ROWS, WIDTH), bf16),
            pltpu.VMEM((ROWS, WIDTH), bf16),
            pltpu.VMEM((LEN, 128), f32),
            pltpu.VMEM((LEN, D_HEAD), f32),
            pltpu.VMEM((LEN, D_HEAD), f32),
            pltpu.VMEM((8, 128), f32),
            pltpu.VMEM((4, 8, 128), f32),
            pltpu.VMEM((12, 8, 128), f32),
            pltpu.VMEM((SLOTS, 8, 128), f32),
            dma((4, 2)), dma((4, 2)), dma((4, 2)), dma((4, 2)), dma((3,)), dma((3,)), dma((8,)),
            pltpu.SemaphoreType.REGULAR, pltpu.SemaphoreType.REGULAR, pltpu.SemaphoreType.REGULAR,
        ],
        compiler_params=pltpu.CompilerParams(
            collective_id=0, has_side_effects=True, vmem_limit_bytes=48 * 2**20
        ),
        name="packed_attention",
    )(
        *[
            pltpu.with_memory_space_constraint(array, pltpu.HBM)
            for array in (
                queries, keys, values, out_grad,
                q_gain.reshape(WIDTH // 128, 128), k_gain.reshape(WIDTH // 128, 128),
                segments, visible,
            )
        ]
    )
    attn_out, query_grad, key_grad, value_grad, gq, gk = pl.pallas_call(
        store,
        out_shape=outs,
        in_specs=[vmem] * 6,
        out_specs=[hbm] * 6,
        scratch_shapes=[dma((6,))],
        compiler_params=pltpu.CompilerParams(vmem_limit_bytes=16 * 2**20),
        name="store",
    )(*made)
    return (attn_out, query_grad, key_grad, value_grad, gq.reshape(WIDTH), gk.reshape(WIDTH))


def solution(mesh):
    finer = Mesh(mesh.devices.reshape(2, 12, 4, 4, 2), ("dp_0", "dp_1", "dp_2", "seq_0", "seq_1"))
    placed = (
        P(DP_SEQ, None),
        P(DP_SEQ, None),
        P(DP_SEQ, None),
        P(),
        P(),
        P(DP_SEQ, None),
        P(DP, None),
        P(DP, None),
    )
    return jax.shard_map(
        per_device,
        mesh=finer,
        in_specs=placed,
        out_specs=(P(DP_SEQ, None), P(DP_SEQ, None), P(DP_SEQ, None), P(DP_SEQ, None), P(), P()),
        check_vma=False,
    )
```

```python
import functools

import jax
import jax.numpy as jnp
from jax import lax
from jax.experimental import pallas as pl
from jax.experimental.pallas import tpu as pltpu
from jax.sharding import Mesh
from jax.sharding import PartitionSpec as P

D_HEAD = 128
DP_SEQ = ("dp_0", "dp_1", "dp_2", "seq_0", "seq_1")
DP = ("dp_0", "dp_1", "dp_2")
MESH = pl.DeviceIdType.MESH

epsilon = 1e-06
N_SEQ = 8
ROWS = 128
LEN = 1024
WIDTH = 2048
BLOCK = 256
SCALE = D_HEAD ** (-0.5)
LOG2E = 1.4426950408889634
SLOTS = 16
ORDER = ((2, 0), (2, 1), (1, 0), (3, 0), (1, 1), (3, 1), (0, 1))


def nt(a, b):
    return lax.dot_general(a, b, (((1,), (1,)), ((), ())), preferred_element_type=jnp.float32)


def tn(a, b):
    return lax.dot_general(a, b, (((0,), (0,)), ((), ())), preferred_element_type=jnp.float32)


def nn(a, b):
    return lax.dot_general(a, b, (((1,), (0,)), ((), ())), preferred_element_type=jnp.float32)


def wide(gain_ref):
    return jnp.concatenate([gain_ref[r : r + 1, :] for r in range(WIDTH // 128)], axis=1)


def kernel(
    q_hbm, k_hbm, v_hbm, g_hbm, qg_hbm, kg_hbm, seg_hbm, vis_hbm,
    o_ref, dq_ref, dk_ref, dv_ref, gq_ref, gk_ref,
    q_ref, k_ref, v_ref, g_ref, qg_ref, kg_ref, seg_ref, vis_ref,
    qn, kn, qi, ki, rx, tx, rdq, rdk, code, acc_k, acc_v, part, gx, gz, gy,
    in_send, in_recv, out_send, out_recv, g_send, g_recv, load_sem, ready, line, go,
):
    ylo, z, x = lax.axis_index("dp_0"), lax.axis_index("dp_1"), lax.axis_index("dp_2")
    chip, core = lax.axis_index("seq_0"), lax.axis_index("seq_1")
    me = chip * 2 + core

    loads = [
        pltpu.make_async_copy(source, target, load_sem.at[i])
        for i, (source, target) in enumerate(
            (
                (qg_hbm, qg_ref), (q_hbm, q_ref), (kg_hbm, kg_ref), (k_hbm, k_ref),
                (v_hbm, v_ref), (g_hbm, g_ref), (seg_hbm, seg_ref), (vis_hbm, vis_ref),
            )
        )
    ]
    for load in loads:
        load.start()

    barrier = pltpu.get_barrier_semaphore()
    leader = me == 0

    def greet(device):
        pl.semaphore_signal(barrier, inc=1, device_id=device, device_id_type=MESH)

    def member(hops, turn):
        at, side = lax.rem(chip + hops, 4), lax.rem(core + turn, 2)
        return at * 2 + side, {"seq_0": at, "seq_1": side}

    members = [member(hops, turn) for hops, turn in ORDER]

    def across(step):
        other = lax.rem(ylo * N_SEQ + me + step, SLOTS)
        return {
            "dp_0": other // N_SEQ,
            "seq_0": lax.rem(other, N_SEQ) // 2,
            "seq_1": lax.rem(other, 2),
        }

    x_peers = [{"dp_2": lax.rem(x + d, 4)} for d in range(1, 4)]
    z_peers = [{"dp_1": lax.rem(z + d, 12)} for d in range(1, 12)]
    y_peers = [across(d) for d in range(1, SLOTS)]
    leaders = x_peers + z_peers + [{"dp_0": 1 - ylo}]
    for other, device in members:

        @pl.when(other != 0)
        def _():
            greet(device)

    @pl.when(leader)
    def _():
        for device in leaders:
            greet(device)

    def normalize(raw_ref, gain, out, inv_ref):
        def rows_of(i, _):
            rows = pl.ds(pl.multiple_of(i * 16, 16), 16)
            raw = raw_ref[rows, :].astype(jnp.float32)
            inv = lax.rsqrt(jnp.mean(raw * raw, axis=-1, keepdims=True) + epsilon)
            inv_ref[rows, :] = jnp.broadcast_to(inv, (16, 128))
            out[rows, :] = (raw * inv * gain).astype(jnp.bfloat16)
            return 0

        lax.fori_loop(0, ROWS // 16, rows_of, 0)

    part[...] = jnp.zeros_like(part)
    loads[0].wait()
    loads[1].wait()
    q_gain = wide(qg_ref)
    normalize(q_ref, q_gain, qn, qi)
    loads[2].wait()
    loads[3].wait()
    k_gain = wide(kg_ref)
    normalize(k_ref, k_gain, kn, ki)
    for load in loads[4:]:
        load.wait()
    sources = (qn, kn, v_ref, g_ref)
    my_rows = pl.ds(pl.multiple_of(me * ROWS, ROWS), ROWS)

    def columns(device, h):
        return pl.ds(pl.multiple_of(device * 256 + h * 128, 128), 128)

    @pl.when(me != 0)
    def _():
        pl.semaphore_wait(barrier, N_SEQ - 1)
        pl.semaphore_signal(
            ready, inc=1, device_id={"seq_0": 0, "seq_1": 0}, device_id_type=MESH
        )

    @pl.when(leader)
    def _():
        pl.semaphore_wait(ready, N_SEQ - 1)

    for h in range(2):
        for a in range(4):
            for other, device in members:
                pltpu.make_async_remote_copy(
                    src_ref=sources[a].at[:, columns(other, h)],
                    dst_ref=rx.at[a, h, my_rows],
                    send_sem=in_send.at[a, h],
                    recv_sem=in_recv.at[a, h],
                    device_id=device,
                    device_id_type=MESH,
                ).start()
    for h in range(2):
        for a in range(4):
            rx[a, h, my_rows, :] = sources[a][:, columns(me, h)]

    seg_row = seg_ref[...].astype(jnp.float32)
    key_row = jnp.where(vis_ref[...] == 1, seg_row, -1.0)
    for j in range(LEN // 128):
        piece = jnp.broadcast_to(key_row[:, j * 128 : (j + 1) * 128], (128, 128))
        code[j * 128 : (j + 1) * 128, :] = piece.T

    @pl.when(leader)
    def _():
        pl.semaphore_wait(barrier, len(leaders))
        for device in leaders:
            pl.semaphore_signal(line, inc=1, device_id=device, device_id_type=MESH)

    def of_all(a, h, sends, recvs):
        return pltpu.make_async_remote_copy(
            src_ref=rx.at[a, h, pl.ds(0, 7 * ROWS)],
            dst_ref=rx.at[a, h, pl.ds(0, 7 * ROWS)],
            send_sem=sends.at[a, h],
            recv_sem=recvs.at[a, h],
            device_id=members[0][1],
            device_id_type=MESH,
        )

    landing = (o_ref, rdq, rdk, dv_ref)

    def send_out(a, h, other):
        pltpu.make_async_remote_copy(
            src_ref=tx.at[a, h, pl.ds(pl.multiple_of(other * ROWS, ROWS), ROWS)],
            dst_ref=landing[a].at[:, columns(me, h)],
            send_sem=out_send.at[a, h],
            recv_sem=out_recv.at[a, h],
            device_id={"seq_0": other // 2, "seq_1": lax.rem(other, 2)},
            device_id_type=MESH,
        ).start()

    def send_all(a, h):
        for other, _ in members:
            send_out(a, h, other)

    def keep_own(a, h):
        landing[a][:, columns(me, h)] = tx[a, h, my_rows, :]

    for h in range(2):
        for a in range(4):
            of_all(a, h, in_send, in_recv).wait_recv()
        if h == 1:
            for a in range(4):
                send_all(a, 0)
        acc_k[...] = jnp.zeros_like(acc_k)
        acc_v[...] = jnp.zeros_like(acc_v)

        def block(t, gain_sum):
            at_chip = lax.rem(chip + 1 + t, 4)
            start = pl.multiple_of(at_chip * BLOCK, BLOCK)
            rows = pl.ds(start, BLOCK)
            q_i, g_i = rx[0, h, rows, :], rx[3, h, rows, :]
            keys, vals = rx[1, h], rx[2, h]
            seg_i = seg_ref[:, rows].astype(jnp.float32)
            k_code = code[...]
            k_code = jnp.concatenate([k_code, k_code], axis=1)
            key_at = lax.broadcasted_iota(jnp.int32, (LEN, BLOCK), 0)
            query_at = lax.broadcasted_iota(jnp.int32, (LEN, BLOCK), 1) + start
            allowed = (k_code == seg_i) | (key_at == query_at)
            scores = jnp.where(allowed, nt(keys, q_i), -1e30)
            top = jnp.max(scores, axis=0, keepdims=True)
            weights = jnp.exp2((scores - top) * (SCALE * LOG2E))
            prob = weights * (1.0 / jnp.sum(weights, axis=0, keepdims=True))
            half = prob.astype(jnp.bfloat16)
            tx[0, h, rows, :] = tn(vals, half).T.astype(jnp.bfloat16)
            dprob = nt(vals, g_i)
            dot = jnp.sum(prob * dprob, axis=0, keepdims=True)
            grad = (prob * (dprob - dot) * SCALE).astype(jnp.bfloat16)
            dq_i = tn(keys, grad).T.astype(jnp.bfloat16)
            tx[1, h, rows, :] = dq_i
            acc_v[...] += nn(half, g_i)
            acc_k[...] += nn(grad, q_i)
            if h == 1:
                for c in range(2):
                    other = at_chip * 2 + c

                    @pl.when(other != me)
                    def _():
                        send_out(0, h, other)
                        send_out(1, h, other)

            return gain_sum + jnp.sum(
                dq_i.astype(jnp.float32) * q_i.astype(jnp.float32), axis=0, keepdims=True
            )

        q_sum = lax.fori_loop(0, LEN // BLOCK, block, jnp.zeros((1, D_HEAD), jnp.float32))
        tx[2, h] = acc_k[...].astype(jnp.bfloat16)
        tx[3, h] = acc_v[...].astype(jnp.bfloat16)
        if h == 1:
            send_all(2, h)
        for a in range(4):
            keep_own(a, h)
        k_sum = jnp.sum(
            tx[2, h].astype(jnp.float32) * rx[1, h].astype(jnp.float32), axis=0, keepdims=True
        )
        if h == 0:

            @pl.when(leader)
            def _():
                pl.semaphore_wait(line, len(leaders))
                for _, device in members:
                    pl.semaphore_signal(go, inc=1, device_id=device, device_id_type=MESH)

        part[h : h + 1, :] = q_sum / qg_ref[pl.ds(me * 2 + h, 1), :]
        part[2 + h : 3 + h, :] = k_sum / kg_ref[pl.ds(me * 2 + h, 1), :]

    def spread(slot, peers, sem):
        copies = []
        for device in peers:
            pltpu.make_async_remote_copy(
                src_ref=slot, dst_ref=slot, send_sem=g_send.at[sem], recv_sem=g_recv.at[sem],
                device_id=device, device_id_type=MESH,
            ).start()

    def settle(slots, peers, sem):
        copy = pltpu.make_async_remote_copy(
            src_ref=slots.at[pl.ds(0, len(peers))], dst_ref=slots.at[pl.ds(0, len(peers))],
            send_sem=g_send.at[sem], recv_sem=g_recv.at[sem],
            device_id=peers[0], device_id_type=MESH,
        )
        copy.wait_recv()
        copy.wait_send()

    @pl.when(me != 0)
    def _():
        pl.semaphore_wait(go, 1)

    gx[x] = part[...]
    spread(gx.at[x], x_peers, 0)
    settle(gx, x_peers, 0)
    gz[z] = (gx[0] + gx[1]) + (gx[2] + gx[3])
    spread(gz.at[z], z_peers, 1)
    settle(gz, z_peers, 1)
    total = gz[0]
    for i in range(1, 12):
        total = total + gz[i]
    slot = ylo * N_SEQ + me
    gy[slot] = total
    spread(gy.at[slot], y_peers, 2)
    send_all(3, 1)

    def norm_back(raw_ref, inv_ref, gain, grads, out):
        def rows_of(i, _):
            rows = pl.ds(pl.multiple_of(i * 16, 16), 16)
            raw = raw_ref[rows, :].astype(jnp.float32)
            inv = inv_ref[rows, :][:, 0:1]
            scaled = gain * grads[rows, :].astype(jnp.float32)
            mean_term = jnp.mean(scaled * raw, axis=-1, keepdims=True)
            out[rows, :] = (inv * scaled - raw * (inv * inv * inv * mean_term)).astype(jnp.bfloat16)
            return 0

        lax.fori_loop(0, ROWS // 16, rows_of, 0)

    for h in range(2):
        of_all(1, h, out_send, out_recv).wait_recv()
    norm_back(q_ref, qi, q_gain, rdq, dq_ref)
    for h in range(2):
        of_all(2, h, out_send, out_recv).wait_recv()
    norm_back(k_ref, ki, k_gain, rdk, dk_ref)
    for a in (0, 3):
        for h in range(2):
            of_all(a, h, out_send, out_recv).wait_recv()
    settle(gy, y_peers, 2)
    for s in range(N_SEQ):
        both = gy[s] + gy[N_SEQ + s]
        gq_ref[2 * s : 2 * s + 2, :] = both[0:2, :]
        gk_ref[2 * s : 2 * s + 2, :] = both[2:4, :]
    for h in range(2):
        for a in range(4):
            of_all(a, h, in_send, in_recv).wait_send()
            of_all(a, h, out_send, out_recv).wait_send()


def store(*refs):
    n = 6
    sources, targets, sem = refs[:n], refs[n : 2 * n], refs[2 * n]
    copies = [pltpu.make_async_copy(sources[i], targets[i], sem.at[i]) for i in range(n)]
    for copy in copies:
        copy.start()
    for copy in copies:
        copy.wait()


def per_device(queries, keys, values, q_gain, k_gain, out_grad, segments, visible):
    vmem = pl.BlockSpec(memory_space=pltpu.VMEM)
    rows = jax.ShapeDtypeStruct((ROWS, WIDTH), jnp.bfloat16)
    gains = jax.ShapeDtypeStruct((WIDTH // 128, 128), jnp.float32)
    dma = pltpu.SemaphoreType.DMA
    bf16, f32 = jnp.bfloat16, jnp.float32
    hbm = pl.BlockSpec(memory_space=pltpu.HBM)
    outs = (rows, rows, rows, rows, gains, gains)
    made = pl.pallas_call(
        kernel,
        out_shape=outs,
        in_specs=[hbm] * 8,
        out_specs=[vmem] * 6,
        scratch_shapes=[
            pltpu.VMEM((ROWS, WIDTH), bf16),
            pltpu.VMEM((ROWS, WIDTH), bf16),
            pltpu.VMEM((ROWS, WIDTH), bf16),
            pltpu.VMEM((ROWS, WIDTH), bf16),
            pltpu.VMEM((WIDTH // 128, 128), f32),
            pltpu.VMEM((WIDTH // 128, 128), f32),
            pltpu.VMEM((1, LEN), jnp.int32),
            pltpu.VMEM((1, LEN), jnp.int32),
            pltpu.VMEM((ROWS, WIDTH), bf16),
            pltpu.VMEM((ROWS, WIDTH), bf16),
            pltpu.VMEM((ROWS, 128), f32),
            pltpu.VMEM((ROWS, 128), f32),
            pltpu.VMEM((4, 2, LEN, D_HEAD), bf16),
            pltpu.VMEM((4, 2, LEN, D_HEAD), bf16),
            pltpu.VMEM((ROWS, WIDTH), bf16),
            pltpu.VMEM((ROWS, WIDTH), bf16),
            pltpu.VMEM((LEN, 128), f32),
            pltpu.VMEM((LEN, D_HEAD), f32),
            pltpu.VMEM((LEN, D_HEAD), f32),
            pltpu.VMEM((8, 128), f32),
            pltpu.VMEM((4, 8, 128), f32),
            pltpu.VMEM((12, 8, 128), f32),
            pltpu.VMEM((SLOTS, 8, 128), f32),
            dma((4, 2)), dma((4, 2)), dma((4, 2)), dma((4, 2)), dma((3,)), dma((3,)), dma((8,)),
            pltpu.SemaphoreType.REGULAR, pltpu.SemaphoreType.REGULAR, pltpu.SemaphoreType.REGULAR,
        ],
        compiler_params=pltpu.CompilerParams(
            collective_id=0, has_side_effects=True, vmem_limit_bytes=48 * 2**20
        ),
        name="packed_attention",
    )(
        *[
            pltpu.with_memory_space_constraint(array, pltpu.HBM)
            for array in (
                queries, keys, values, out_grad,
                q_gain.reshape(WIDTH // 128, 128), k_gain.reshape(WIDTH // 128, 128),
                segments, visible,
            )
        ]
    )
    attn_out, query_grad, key_grad, value_grad, gq, gk = pl.pallas_call(
        store,
        out_shape=outs,
        in_specs=[vmem] * 6,
        out_specs=[hbm] * 6,
        scratch_shapes=[dma((6,))],
        compiler_params=pltpu.CompilerParams(vmem_limit_bytes=16 * 2**20),
        name="store",
    )(*made)
    return (attn_out, query_grad, key_grad, value_grad, gq.reshape(WIDTH), gk.reshape(WIDTH))


def solution(mesh):
    finer = Mesh(mesh.devices.reshape(2, 12, 4, 4, 2), ("dp_0", "dp_1", "dp_2", "seq_0", "seq_1"))
    placed = (
        P(DP_SEQ, None),
        P(DP_SEQ, None),
        P(DP_SEQ, None),
        P(),
        P(),
        P(DP_SEQ, None),
        P(DP, None),
        P(DP, None),
    )
    return jax.shard_map(
        per_device,
        mesh=finer,
        in_specs=placed,
        out_specs=(P(DP_SEQ, None), P(DP_SEQ, None), P(DP_SEQ, None), P(DP_SEQ, None), P(), P()),
        check_vma=False,
    )
```

```python
import functools

import jax
import jax.numpy as jnp
from jax import lax
from jax.experimental import pallas as pl
from jax.experimental.pallas import tpu as pltpu
from jax.sharding import Mesh
from jax.sharding import PartitionSpec as P

D_HEAD = 128
DP_SEQ = ("dp_0", "dp_1", "dp_2", "seq_0", "seq_1")
DP = ("dp_0", "dp_1", "dp_2")
MESH = pl.DeviceIdType.MESH

epsilon = 1e-06
N_SEQ = 8
ROWS = 128
LEN = 1024
WIDTH = 2048
BLOCK = 256
SCALE = D_HEAD ** (-0.5)
LOG2E = 1.4426950408889634
SLOTS = 16
ORDER = ((2, 0), (2, 1), (1, 0), (3, 0), (1, 1), (3, 1), (0, 1))


def nt(a, b):
    return lax.dot_general(a, b, (((1,), (1,)), ((), ())), preferred_element_type=jnp.float32)


def tn(a, b):
    return lax.dot_general(a, b, (((0,), (0,)), ((), ())), preferred_element_type=jnp.float32)


def nn(a, b):
    return lax.dot_general(a, b, (((1,), (0,)), ((), ())), preferred_element_type=jnp.float32)


def wide(gain_ref):
    return jnp.concatenate([gain_ref[r : r + 1, :] for r in range(WIDTH // 128)], axis=1)


def kernel(
    q_hbm, k_hbm, v_hbm, g_hbm, qg_hbm, kg_hbm, seg_hbm, vis_hbm,
    o_ref, dq_ref, dk_ref, dv_ref, gq_ref, gk_ref,
    q_ref, k_ref, v_ref, g_ref, qg_ref, kg_ref, seg_ref, vis_ref,
    qn, kn, qi, ki, rx, tx, rdq, rdk, code, acc_k, acc_v, part, gx, gz, gy,
    in_send, in_recv, out_send, out_recv, g_send, g_recv, load_sem, ready, line, go,
):
    ylo, z, x = lax.axis_index("dp_0"), lax.axis_index("dp_1"), lax.axis_index("dp_2")
    chip, core = lax.axis_index("seq_0"), lax.axis_index("seq_1")
    me = chip * 2 + core

    loads = [
        pltpu.make_async_copy(source, target, load_sem.at[i])
        for i, (source, target) in enumerate(
            (
                (qg_hbm, qg_ref), (q_hbm, q_ref), (kg_hbm, kg_ref), (k_hbm, k_ref),
                (v_hbm, v_ref), (g_hbm, g_ref), (seg_hbm, seg_ref), (vis_hbm, vis_ref),
            )
        )
    ]
    for load in loads:
        load.start()

    barrier = pltpu.get_barrier_semaphore()
    leader = me == 0

    def greet(device):
        pl.semaphore_signal(barrier, inc=1, device_id=device, device_id_type=MESH)

    def member(hops, turn):
        at, side = lax.rem(chip + hops, 4), lax.rem(core + turn, 2)
        return at * 2 + side, {"seq_0": at, "seq_1": side}

    members = [member(hops, turn) for hops, turn in ORDER]

    def across(step):
        other = lax.rem(ylo * N_SEQ + me + step, SLOTS)
        return {
            "dp_0": other // N_SEQ,
            "seq_0": lax.rem(other, N_SEQ) // 2,
            "seq_1": lax.rem(other, 2),
        }

    x_peers = [{"dp_2": lax.rem(x + d, 4)} for d in range(1, 4)]
    z_peers = [{"dp_1": lax.rem(z + d, 12)} for d in range(1, 12)]
    y_peers = [across(d) for d in range(1, SLOTS)]
    leaders = x_peers + z_peers + [{"dp_0": 1 - ylo}]
    for other, device in members:

        @pl.when(other != 0)
        def _():
            greet(device)

    @pl.when(leader)
    def _():
        for device in leaders:
            greet(device)

    def normalize(raw_ref, gain, out, inv_ref):
        def rows_of(i, _):
            rows = pl.ds(pl.multiple_of(i * 16, 16), 16)
            raw = raw_ref[rows, :].astype(jnp.float32)
            inv = lax.rsqrt(jnp.mean(raw * raw, axis=-1, keepdims=True) + epsilon)
            inv_ref[rows, :] = jnp.broadcast_to(inv, (16, 128))
            out[rows, :] = (raw * inv * gain).astype(jnp.bfloat16)
            return 0

        lax.fori_loop(0, ROWS // 16, rows_of, 0)

    loads[0].wait()
    loads[1].wait()
    q_gain = wide(qg_ref)
    normalize(q_ref, q_gain, qn, qi)
    loads[2].wait()
    loads[3].wait()
    k_gain = wide(kg_ref)
    normalize(k_ref, k_gain, kn, ki)
    for load in loads[4:]:
        load.wait()
    sources = (qn, kn, v_ref, g_ref)
    my_rows = pl.ds(pl.multiple_of(me * ROWS, ROWS), ROWS)

    def columns(device, h):
        return pl.ds(pl.multiple_of(device * 256 + h * 128, 128), 128)

    @pl.when(me != 0)
    def _():
        pl.semaphore_wait(barrier, N_SEQ - 1)
        pl.semaphore_signal(
            ready, inc=1, device_id={"seq_0": 0, "seq_1": 0}, device_id_type=MESH
        )

    @pl.when(leader)
    def _():
        pl.semaphore_wait(ready, N_SEQ - 1)

    for h in range(2):
        for a in range(4):
            for other, device in members:
                pltpu.make_async_remote_copy(
                    src_ref=sources[a].at[:, columns(other, h)],
                    dst_ref=rx.at[a, h, my_rows],
                    send_sem=in_send.at[a, h],
                    recv_sem=in_recv.at[a, h],
                    device_id=device,
                    device_id_type=MESH,
                ).start()
    for h in range(2):
        for a in range(4):
            rx[a, h, my_rows, :] = sources[a][:, columns(me, h)]

    seg_row = seg_ref[...].astype(jnp.float32)
    key_row = jnp.where(vis_ref[...] == 1, seg_row, -1.0)
    for j in range(LEN // 128):
        piece = jnp.broadcast_to(key_row[:, j * 128 : (j + 1) * 128], (128, 128))
        code[j * 128 : (j + 1) * 128, :] = piece.T

    @pl.when(leader)
    def _():
        pl.semaphore_wait(barrier, len(leaders))
        for device in leaders:
            pl.semaphore_signal(line, inc=1, device_id=device, device_id_type=MESH)

    def of_all(a, h, sends, recvs):
        return pltpu.make_async_remote_copy(
            src_ref=rx.at[a, h, pl.ds(0, 7 * ROWS)],
            dst_ref=rx.at[a, h, pl.ds(0, 7 * ROWS)],
            send_sem=sends.at[a, h],
            recv_sem=recvs.at[a, h],
            device_id=members[0][1],
            device_id_type=MESH,
        )

    landing = (o_ref, rdq, rdk, dv_ref)

    def send_out(a, h, other):
        pltpu.make_async_remote_copy(
            src_ref=tx.at[a, h, pl.ds(pl.multiple_of(other * ROWS, ROWS), ROWS)],
            dst_ref=landing[a].at[:, columns(me, h)],
            send_sem=out_send.at[a, h],
            recv_sem=out_recv.at[a, h],
            device_id={"seq_0": other // 2, "seq_1": lax.rem(other, 2)},
            device_id_type=MESH,
        ).start()

    def send_all(a, h):
        for other, _ in members:
            send_out(a, h, other)

    def keep_own(a, h):
        landing[a][:, columns(me, h)] = tx[a, h, my_rows, :]

    for h in range(2):
        for a in range(4):
            of_all(a, h, in_send, in_recv).wait_recv()
        if h == 1:
            for a in range(4):
                send_all(a, 0)
        acc_k[...] = jnp.zeros_like(acc_k)
        acc_v[...] = jnp.zeros_like(acc_v)

        def block(t, gain_sum):
            at_chip = lax.rem(chip + 1 + t, 4)
            start = pl.multiple_of(at_chip * BLOCK, BLOCK)
            rows = pl.ds(start, BLOCK)
            q_i, g_i = rx[0, h, rows, :], rx[3, h, rows, :]
            keys, vals = rx[1, h], rx[2, h]
            seg_i = seg_ref[:, rows].astype(jnp.float32)
            k_code = code[...]
            k_code = jnp.concatenate([k_code, k_code], axis=1)
            key_at = lax.broadcasted_iota(jnp.int32, (LEN, BLOCK), 0)
            query_at = lax.broadcasted_iota(jnp.int32, (LEN, BLOCK), 1) + start
            allowed = (k_code == seg_i) | (key_at == query_at)
            scores = jnp.where(allowed, nt(keys, q_i), -1e30)
            top = jnp.max(scores, axis=0, keepdims=True)
            weights = jnp.exp2((scores - top) * (SCALE * LOG2E))
            prob = weights * (1.0 / jnp.sum(weights, axis=0, keepdims=True))
            half = prob.astype(jnp.bfloat16)
            tx[0, h, rows, :] = tn(vals, half).T.astype(jnp.bfloat16)
            dprob = nt(vals, g_i)
            dot = jnp.sum(prob * dprob, axis=0, keepdims=True)
            grad = (prob * (dprob - dot) * SCALE).astype(jnp.bfloat16)
            dq_i = tn(keys, grad).T.astype(jnp.bfloat16)
            tx[1, h, rows, :] = dq_i
            acc_v[...] += nn(half, g_i)
            acc_k[...] += nn(grad, q_i)
            if h == 1:
                for c in range(2):
                    other = at_chip * 2 + c

                    @pl.when(other != me)
                    def _():
                        send_out(0, h, other)
                        send_out(1, h, other)

            return gain_sum + jnp.sum(
                dq_i.astype(jnp.float32) * q_i.astype(jnp.float32), axis=0, keepdims=True
            )

        q_sum = lax.fori_loop(0, LEN // BLOCK, block, jnp.zeros((1, D_HEAD), jnp.float32))
        tx[2, h] = acc_k[...].astype(jnp.bfloat16)
        tx[3, h] = acc_v[...].astype(jnp.bfloat16)
        if h == 1:
            send_all(2, h)
        for a in range(4):
            keep_own(a, h)
        k_sum = jnp.sum(
            tx[2, h].astype(jnp.float32) * rx[1, h].astype(jnp.float32), axis=0, keepdims=True
        )
        if h == 0:

            @pl.when(leader)
            def _():
                pl.semaphore_wait(line, len(leaders))
                for _, device in members:
                    pl.semaphore_signal(go, inc=1, device_id=device, device_id_type=MESH)

        part[h : h + 1, :] = q_sum / qg_ref[pl.ds(me * 2 + h, 1), :]
        part[2 + h : 3 + h, :] = k_sum / kg_ref[pl.ds(me * 2 + h, 1), :]

    def spread(slot, peers, sem):
        copies = []
        for device in peers:
            pltpu.make_async_remote_copy(
                src_ref=slot, dst_ref=slot, send_sem=g_send.at[sem], recv_sem=g_recv.at[sem],
                device_id=device, device_id_type=MESH,
            ).start()

    def settle(slots, peers, sem):
        copy = pltpu.make_async_remote_copy(
            src_ref=slots.at[pl.ds(0, len(peers))], dst_ref=slots.at[pl.ds(0, len(peers))],
            send_sem=g_send.at[sem], recv_sem=g_recv.at[sem],
            device_id=peers[0], device_id_type=MESH,
        )
        copy.wait_recv()
        copy.wait_send()

    @pl.when(me != 0)
    def _():
        pl.semaphore_wait(go, 1)

    gx[x] = part[...]
    spread(gx.at[x], x_peers, 0)
    settle(gx, x_peers, 0)
    gz[z] = (gx[0] + gx[1]) + (gx[2] + gx[3])
    spread(gz.at[z], z_peers, 1)
    settle(gz, z_peers, 1)
    total = gz[0]
    for i in range(1, 12):
        total = total + gz[i]
    slot = ylo * N_SEQ + me
    gy[slot] = total
    spread(gy.at[slot], y_peers, 2)
    send_all(3, 1)

    def norm_back(raw_ref, inv_ref, gain, grads, out):
        def rows_of(i, _):
            rows = pl.ds(pl.multiple_of(i * 16, 16), 16)
            raw = raw_ref[rows, :].astype(jnp.float32)
            inv = inv_ref[rows, :][:, 0:1]
            scaled = gain * grads[rows, :].astype(jnp.float32)
            mean_term = jnp.mean(scaled * raw, axis=-1, keepdims=True)
            out[rows, :] = (inv * scaled - raw * (inv * inv * inv * mean_term)).astype(jnp.bfloat16)
            return 0

        lax.fori_loop(0, ROWS // 16, rows_of, 0)

    for h in range(2):
        of_all(1, h, out_send, out_recv).wait_recv()
    norm_back(q_ref, qi, q_gain, rdq, dq_ref)
    for h in range(2):
        of_all(2, h, out_send, out_recv).wait_recv()
    norm_back(k_ref, ki, k_gain, rdk, dk_ref)
    for a in (0, 3):
        for h in range(2):
            of_all(a, h, out_send, out_recv).wait_recv()
    settle(gy, y_peers, 2)
    for s in range(N_SEQ):
        both = gy[s] + gy[N_SEQ + s]
        gq_ref[2 * s : 2 * s + 2, :] = both[0:2, :]
        gk_ref[2 * s : 2 * s + 2, :] = both[2:4, :]
    for h in range(2):
        for a in range(4):
            of_all(a, h, in_send, in_recv).wait_send()
            of_all(a, h, out_send, out_recv).wait_send()


def store(*refs):
    n = 6
    sources, targets, sem = refs[:n], refs[n : 2 * n], refs[2 * n]
    copies = [pltpu.make_async_copy(sources[i], targets[i], sem.at[i]) for i in range(n)]
    for copy in copies:
        copy.start()
    for copy in copies:
        copy.wait()


def per_device(queries, keys, values, q_gain, k_gain, out_grad, segments, visible):
    vmem = pl.BlockSpec(memory_space=pltpu.VMEM)
    rows = jax.ShapeDtypeStruct((ROWS, WIDTH), jnp.bfloat16)
    gains = jax.ShapeDtypeStruct((WIDTH // 128, 128), jnp.float32)
    dma = pltpu.SemaphoreType.DMA
    bf16, f32 = jnp.bfloat16, jnp.float32
    hbm = pl.BlockSpec(memory_space=pltpu.HBM)
    outs = (rows, rows, rows, rows, gains, gains)
    made = pl.pallas_call(
        kernel,
        out_shape=outs,
        in_specs=[hbm] * 8,
        out_specs=[vmem] * 6,
        scratch_shapes=[
            pltpu.VMEM((ROWS, WIDTH), bf16),
            pltpu.VMEM((ROWS, WIDTH), bf16),
            pltpu.VMEM((ROWS, WIDTH), bf16),
            pltpu.VMEM((ROWS, WIDTH), bf16),
            pltpu.VMEM((WIDTH // 128, 128), f32),
            pltpu.VMEM((WIDTH // 128, 128), f32),
            pltpu.VMEM((1, LEN), jnp.int32),
            pltpu.VMEM((1, LEN), jnp.int32),
            pltpu.VMEM((ROWS, WIDTH), bf16),
            pltpu.VMEM((ROWS, WIDTH), bf16),
            pltpu.VMEM((ROWS, 128), f32),
            pltpu.VMEM((ROWS, 128), f32),
            pltpu.VMEM((4, 2, LEN, D_HEAD), bf16),
            pltpu.VMEM((4, 2, LEN, D_HEAD), bf16),
            pltpu.VMEM((ROWS, WIDTH), bf16),
            pltpu.VMEM((ROWS, WIDTH), bf16),
            pltpu.VMEM((LEN, 128), f32),
            pltpu.VMEM((LEN, D_HEAD), f32),
            pltpu.VMEM((LEN, D_HEAD), f32),
            pltpu.VMEM((4, 128), f32),
            pltpu.VMEM((4, 4, 128), f32),
            pltpu.VMEM((12, 4, 128), f32),
            pltpu.VMEM((SLOTS, 4, 128), f32),
            dma((4, 2)), dma((4, 2)), dma((4, 2)), dma((4, 2)), dma((3,)), dma((3,)), dma((8,)),
            pltpu.SemaphoreType.REGULAR, pltpu.SemaphoreType.REGULAR, pltpu.SemaphoreType.REGULAR,
        ],
        compiler_params=pltpu.CompilerParams(
            collective_id=0, has_side_effects=True, vmem_limit_bytes=48 * 2**20
        ),
        name="packed_attention",
    )(
        *[
            pltpu.with_memory_space_constraint(array, pltpu.HBM)
            for array in (
                queries, keys, values, out_grad,
                q_gain.reshape(WIDTH // 128, 128), k_gain.reshape(WIDTH // 128, 128),
                segments, visible,
            )
        ]
    )
    attn_out, query_grad, key_grad, value_grad, gq, gk = pl.pallas_call(
        store,
        out_shape=outs,
        in_specs=[vmem] * 6,
        out_specs=[hbm] * 6,
        scratch_shapes=[dma((6,))],
        compiler_params=pltpu.CompilerParams(vmem_limit_bytes=16 * 2**20),
        name="store",
    )(*made)
    return (attn_out, query_grad, key_grad, value_grad, gq.reshape(WIDTH), gk.reshape(WIDTH))


def solution(mesh):
    finer = Mesh(mesh.devices.reshape(2, 12, 4, 4, 2), ("dp_0", "dp_1", "dp_2", "seq_0", "seq_1"))
    placed = (
        P(DP_SEQ, None),
        P(DP_SEQ, None),
        P(DP_SEQ, None),
        P(),
        P(),
        P(DP_SEQ, None),
        P(DP, None),
        P(DP, None),
    )
    return jax.shard_map(
        per_device,
        mesh=finer,
        in_specs=placed,
        out_specs=(P(DP_SEQ, None), P(DP_SEQ, None), P(DP_SEQ, None), P(DP_SEQ, None), P(), P()),
        check_vma=False,
    )
```
